32 devices in a mesh: gx: 2 (over core), gy: 4 (over y, x), gz: 4 (over z).
Axes of the slice: x: 2, y: 2, z: 4, core: 2. Of those that a mesh axis runs over, the one named last changes fastest.
Arguments:
- velocity: float32 [3, 16, 64, 512], P(None, 'gx', 'gy', 'gz'), may hold values from -6 to 6
- diffusion: float32 [3], replicated, may hold values from 0.5 to 4
Outputs:
- viscous_velocity: float32 [3, 16, 64, 512], P(None, 'gx', 'gy', 'gz')
- residual: float32 [3, 16, 64, 512], P(None, 'gx', 'gy', 'gz')
The draws below stay inside these ranges and needn't reach their ends.
All inputs are finite; a program needn't handle non-finite values.
Results may differ from the reference program's by a relative error of at most 0.0003.
Values sent between devices are 32-bit elements; how exact they have to be, the bound alone decides.
A program may use at most 64 MiB of HBM per device.

```python
import math
import jax
import jax.numpy as jnp

ITERS = 3
NX = 16
NY = 64
NZ = 512


def level_of(stream_key, shape, cuts, least, top_value):
    def one(axis_at, parts):
        draws = jax.random.uniform(jax.random.fold_in(jax.random.fold_in(stream_key, 6), axis_at), (parts,), jnp.float32, least / len(cuts), top_value / len(cuts))
        return jnp.repeat(jnp.exp(draws), shape[axis_at] // parts).reshape((-1,) + (1,) * (len(shape) - axis_at - 1))

    loudness = one(*cuts[0])
    for cut in cuts[1:]:
        loudness = loudness * one(*cut)
    return loudness


def bell_draw(own_key, extent, width, limit, pieces=(), kind=jnp.bfloat16):
    result = width * jax.random.normal(own_key, extent, jnp.float32)
    if pieces:
        result = result * level_of(own_key, extent, pieces, -0.22, 0.18)
    return jnp.clip(result, -limit, limit).astype(kind)


def setup_inputs(seed: int = 0) -> dict:
    key_list = jax.random.split(jax.random.key(seed), 3)
    return {
        "velocity": bell_draw(key_list[0], (3, NX, NY, NZ), 1.0, 6.0, ((1, 2), (2, 4), (3, 4)), jnp.float32),
        "diffusion": jnp.clip(jnp.exp(jax.random.uniform(key_list[1], (3,), jnp.float32, math.log(0.5), math.log(4.0))), 0.5, 4.0),
    }


time_step = 0.25


def trimmed(array, axis, offset):
    index = [slice(None)] + [slice(1, -1)] * 3
    index[axis + 1] = slice(1 + offset, array.shape[axis + 1] - 1 + offset)
    return array[tuple(index)]


def advection(padded):
    total = None
    for axis in range(3):
        flux = padded[axis:axis + 1] * padded
        term = (trimmed(flux, axis, 1) - trimmed(flux, axis, -1)) * 0.5
        total = term if total is None else total + term
    return total


def operate(field, coefficient):
    padded = jnp.pad(field, ((0, 0), (1, 1), (1, 1), (1, 1)))
    beside = padded[:, 2:, 1:-1, 1:-1] + padded[:, :-2, 1:-1, 1:-1]
    beside = beside + padded[:, 1:-1, 2:, 1:-1] + padded[:, 1:-1, :-2, 1:-1]
    beside = beside + padded[:, 1:-1, 1:-1, 2:] + padded[:, 1:-1, 1:-1, :-2]
    return (1.0 + 6.0 * coefficient) * field - coefficient * beside


def inner(first, second):
    return jnp.sum(first * second, axis=(1, 2, 3))[:, None, None, None]


def reference(velocity, diffusion):
    coefficient = diffusion[:, None, None, None]
    padded = jnp.pad(velocity, ((0, 0), (1, 1), (1, 1), (1, 1)))
    section = velocity - time_step * advection(padded)
    solution = jnp.zeros_like(section)
    residual = section
    direction = section
    norm_now = inner(residual, residual)
    for iteration in range(ITERS):
        image = operate(direction, coefficient)
        step_size = norm_now / inner(direction, image)
        solution = solution + step_size * direction
        residual = residual - step_size * image
        norm_next = inner(residual, residual)
        direction = residual + (norm_next / norm_now) * direction
        norm_now = norm_next
    return solution, residual
```

```python
import functools
import itertools

import jax
import jax.numpy as jnp
from jax import lax
from jax.experimental import pallas as pl
from jax.experimental.pallas import tpu as pltpu
from jax.sharding import PartitionSpec as P

AXES = ("gx", "gy", "gz")
MESH_IDS = pl.DeviceIdType.MESH
MARGIN = 4
PAIRS = ((0, 0), (0, 1), (1, 1), (0, 2), (1, 2), (2, 2), (2, 3))
time_step = 0.25
ONE_SHOT = 64


def around(sizes, moved):
    return tuple(lax.rem(lax.axis_index(a) + o, s) for a, o, s in zip(AXES, moved, sizes))


def groups_of(sizes):
    total = sizes[0] * sizes[1] * sizes[2]
    if total <= ONE_SHOT:
        return [(0, 1, 2)]
    return [(0,), (1,), (2,)]


def offsets_of(sizes, group):
    ranges = [range(sizes[k]) if k in group else range(1) for k in range(3)]
    return [o for o in itertools.product(*ranges) if any(o)]


def slot_of(sizes, group):
    slot = 0
    for k in group:
        slot = slot * sizes[k] + lax.axis_index(AXES[k])
    return slot


def kernel(sizes, diff_ref, v_ref, x_ref, r_ref, F, S0, S1, S2, S3, mask, SL, SH, RL, RH, pack, zlow, zhigh, Q, QR, row, *rest):
    groups = groups_of(sizes)
    gathered, (fs, fr, gs, gr) = rest[: len(groups)], rest[len(groups):]
    comps, X, Y, Z = v_ref.shape
    XR, YR, ZR = X + 2 * MARGIN, Y + 2 * MARGIN, 2 * Z
    tiles = Y // 8
    here = [lax.axis_index(a) for a in AXES]

    def exists(moved):
        ok = None
        for k in range(3):
            if moved[k]:
                place = here[k] + moved[k]
                one = (place >= 0) & (place < sizes[k])
                ok = one if ok is None else ok & one
        return ok

    peers = set()
    for group in groups:
        peers.update(offsets_of(sizes, group))
    for dx, dy in itertools.product((-1, 0, 1), (-1, 0, 1)):
        moved = (dx % sizes[0], dy % sizes[1], 0)
        if any(moved):
            peers.add(moved)
    peers = sorted(peers)
    barrier = pltpu.get_barrier_semaphore()

    for c in range(comps):
        F[c, X:XR, 0:Y, 0:Z] = jnp.zeros((XR - X, Y, Z), jnp.float32)
        F[c, X:XR, :, Z:ZR] = jnp.zeros((XR - X, YR, Z), jnp.float32)
    RL[...] = jnp.zeros_like(RL)
    RH[...] = jnp.zeros_like(RH)
    QR[...] = jnp.zeros_like(QR)
    zlow[...] = jnp.zeros_like(zlow)
    zhigh[...] = jnp.zeros_like(zhigh)
    for moved in peers:
        pl.semaphore_signal(barrier, inc=1, device_id=around(sizes, moved), device_id_type=MESH_IDS)

    lane = lax.broadcasted_iota(jnp.int32, (8, Z), 1)
    sub = lax.broadcasted_iota(jnp.int32, (8, Z), 0)
    for c in range(comps):
        packed = jnp.zeros((8, Z), jnp.float32)
        for x in range(X):
            for t in range(tiles):
                g = x * tiles + t
                rolled = pltpu.roll(v_ref[c, x, 8 * t : 8 * t + 8, :], (8 * g + MARGIN) % Z, 1)
                packed = jnp.where(lane // 8 == g, rolled, packed)
        pack[c] = packed
        SL[c] = v_ref[c, :, 0:MARGIN, :]
        SH[c] = v_ref[c, :, Y - MARGIN : Y, :]
    pl.semaphore_wait(barrier, len(peers))

    copies = []

    def send(src, dst, moved):
        k = len(copies)
        copy = pltpu.make_async_remote_copy(
            src_ref=src, dst_ref=dst, send_sem=fs.at[k], recv_sem=fr.at[k],
            device_id=tuple(h + m for h, m in zip(here, moved)), device_id_type=MESH_IDS,
        )
        copies.append((copy, moved))
        pl.when(exists(moved))(copy.start)

    def received(which):
        for copy, moved in which:
            pl.when(exists(tuple(-m for m in moved)))(copy.wait_recv)

    send(pack, zhigh, (0, 0, -1))
    send(pack, zlow, (0, 0, 1))
    z_copies = copies[:]
    send(SL, RH.at[:, 0:X], (0, -1, 0))
    send(SH, RL.at[:, 0:X], (0, 1, 0))
    D = MARGIN - 1
    for dx in (-1, 1):
        planes = pl.ds(0, D) if dx < 0 else pl.ds(X - D, D)
        landing = pl.ds(X, D) if dx < 0 else pl.ds(XR - D, D)
        send(SL.at[:, planes], RH.at[:, landing], (dx, -1, 0))
        send(SH.at[:, planes], RL.at[:, landing], (dx, 1, 0))
    send(v_ref.at[:, 0:MARGIN], F.at[:, X : X + MARGIN, 0:Y, 0:Z], (-1, 0, 0))
    send(v_ref.at[:, X - MARGIN : X], F.at[:, X + MARGIN : XR, 0:Y, 0:Z], (1, 0, 0))
    face_copies = copies[len(z_copies):]

    for c in range(comps):
        F[c, 0:X, 0:Y, 0:Z] = v_ref[c]
    yy = lax.broadcasted_iota(jnp.int32, (YR, ZR), 0)
    zz = lax.broadcasted_iota(jnp.int32, (YR, ZR), 1)
    yy = jnp.where(yy >= Y + MARGIN, yy - YR, yy) + here[1] * Y
    zz = jnp.where(zz >= Z + Z // 2, zz - ZR, zz) + here[2] * Z
    inside = (yy >= 0) & (yy < Y * sizes[1]) & (zz >= 0) & (zz < Z * sizes[2])
    mask[...] = jnp.where(inside, 1.0, 0.0).astype(jnp.float32)

    received(z_copies)
    for c in range(comps):
        Q[c] = jnp.where(lane % 8 < MARGIN, zlow[c], zhigh[c])
    steps = [m for m in itertools.product((-1, 0, 1), (-1, 0, 1)) if any(m)]
    for dx, dy in sorted(steps, key=lambda m: -abs(m[1])):
        send(Q, QR.at[(1 - dx) * 3 + (1 - dy)], (dx, dy, 0))
    q_copies = copies[len(z_copies) + len(face_copies):]
    own = 4
    for c in range(comps):
        for x in range(X):
            for t in range(tiles):
                g = x * tiles + t
                F[c, x, 8 * t : 8 * t + 8, Z:ZR] = pltpu.roll(Q[c], (Z - MARGIN - 8 * g) % Z, 1)

    received(face_copies)
    rows_of_y = [x for x in range(XR) if x < X + D or x >= XR - D]
    for c in range(comps):
        for x in rows_of_y:
            F[c, x, Y : Y + MARGIN, 0:Z] = RH[c, x]
            F[c, x, Y + MARGIN : YR, 0:Z] = RL[c, x]
        for x in (X + D, XR - D - 1):
            F[c, x, Y:YR, 0:Z] = jnp.zeros((YR - Y, Z), jnp.float32)
    received(q_copies)

    for c in range(comps):
        for x in rows_of_y:
            dx, at = (0, x) if x < X else ((1, x - X) if x < X + D else (-1, x - MARGIN - MARGIN))
            base = (dx + 1) * 3 + 1
            if dx:
                for t in range(tiles):
                    g = at * tiles + t
                    F[c, x, 8 * t : 8 * t + 8, Z:ZR] = pltpu.roll(QR[base, c], (Z - MARGIN - 8 * g) % Z, 1)
            above = pltpu.roll(QR[base + 1, c], (Z - MARGIN - 8 * (at * tiles)) % Z, 1)
            below = pltpu.roll(QR[base - 1, c], (Z - MARGIN - 8 * (at * tiles + tiles - 1)) % Z, 1)
            F[c, x, Y:YR, Z:ZR] = jnp.where(sub < MARGIN, above, below)

    def ring(i):
        return lax.rem(i, XR)

    def plane_mask(i):
        place = here[0] * X + i
        xin = (place >= XR) & (place < X * sizes[0] + XR)
        return mask[...] * jnp.where(xin, 1.0, 0.0).astype(jnp.float32)

    def section_plane(i, carry):
        at, after, before = ring(i), ring(i + 1), ring(i - 1)
        inner = plane_mask(i)
        v = [F[c, at] for c in range(comps)]
        va = [F[c, after] for c in range(comps)]
        vb = [F[c, before] for c in range(comps)]
        for c in range(comps):
            total = va[0] * va[c] - vb[0] * vb[c]
            fy = v[1] * v[c]
            total = total + (pltpu.roll(fy, YR - 1, 0) - pltpu.roll(fy, 1, 0))
            fz = v[2] * v[c]
            total = total + (pltpu.roll(fz, ZR - 1, 1) - pltpu.roll(fz, 1, 1))
            S0[c, at] = (v[c] - (0.5 * time_step) * total) * inner
        return carry

    lax.fori_loop(XR - D, XR + X + D, section_plane, 0)

    def beside(ref, c, i):
        f = ref[c, ring(i)]
        total = ref[c, ring(i + 1)] + ref[c, ring(i - 1)]
        total = total + (pltpu.roll(f, YR - 1, 0) + pltpu.roll(f, 1, 0))
        return total + (pltpu.roll(f, ZR - 1, 1) + pltpu.roll(f, 1, 1))

    def first_plane(i, carry):
        inner = plane_mask(i)
        for c in range(comps):
            S1[c, ring(i)] = beside(S0, c, i) * inner
        return carry

    lax.fori_loop(XR - 2, XR + X + 2, first_plane, 0)

    def second_plane(i, carry):
        inner = plane_mask(i)
        for c in range(comps):
            S2[c, ring(i)] = beside(S1, c, i) * inner - 6.0 * S0[c, ring(i)]
        return carry

    lax.fori_loop(XR - 1, XR + X + 1, second_plane, 0)

    def third_plane(i, sums):
        sums = list(sums)
        at = i - XR
        for c in range(comps):
            p = [S[c, at, 0:Y, 0:Z] for S in (S0, S1, S2)]
            p.append(beside(S2, c, i)[0:Y, 0:Z] - 9.0 * p[1])
            S3[c, at] = p[3]
            for k, (a, b) in enumerate(PAIRS):
                both = p[a] * p[b]
                part = both[0:8]
                for t in range(1, tiles):
                    part = part + both[8 * t : 8 * t + 8]
                sums[k * comps + c] = sums[k * comps + c] + part
        return tuple(sums)

    sums = lax.fori_loop(XR, XR + X, third_plane, (jnp.zeros((8, Z), jnp.float32),) * (comps * len(PAIRS)))
    line = jnp.zeros((8, Z), jnp.float32)
    for k, part in enumerate(sums):
        line = jnp.where(lane == k, jnp.sum(part, axis=1, keepdims=True), line)
    line = jnp.sum(line, axis=0, keepdims=True)

    order = 0
    for group, landing in zip(groups, gathered):
        mine = slot_of(sizes, group)
        row[...] = line
        landing[mine] = line
        offsets = offsets_of(sizes, group)
        for moved in offsets:
            pltpu.make_async_remote_copy(
                src_ref=row, dst_ref=landing.at[mine], send_sem=gs.at[order], recv_sem=gr.at[order],
                device_id=around(sizes, moved), device_id_type=MESH_IDS,
            ).start()
        many = landing.at[pl.ds(0, len(offsets))]
        pltpu.make_async_copy(many, many, gr.at[order]).wait()
        line = landing[0]
        for k in range(1, len(offsets) + 1):
            line = line + landing[k]
        pltpu.make_async_copy(many, many, gs.at[order]).wait()
        order += 1

    g = {}
    for k, (a, b) in enumerate(PAIRS):
        value = line if k == 0 else pltpu.roll(line, Z - k * comps, 1)
        g[a, b] = g[b, a] = value
    g[0, 3] = g[1, 2] - 9.0 * g[0, 1]
    g[1, 3] = g[2, 2] + 6.0 * g[0, 2] - 9.0 * g[1, 1]
    at_lane = lax.broadcasted_iota(jnp.int32, (1, Z), 1)
    coef = jnp.full((1, Z), 1.0, jnp.float32)
    for c in range(comps):
        coef = jnp.where(at_lane == c, diff_ref[c], coef)
    diagonal = 1.0 + 6.0 * coef
    zero = jnp.zeros((1, Z), jnp.float32)

    def image_of(d):
        return [
            diagonal * d[0] - 6.0 * coef * d[1],
            diagonal * d[1] - coef * (d[0] + 9.0 * d[2]),
            diagonal * d[2] - coef * d[1],
            -coef * d[2],
        ]

    def form(a, b):
        total = None
        for i, left in enumerate(a):
            for j, right in enumerate(b):
                if left is zero or right is zero:
                    continue
                term = left * right * g[i, j]
                total = term if total is None else total + term
        return total

    res = [zero + 1.0, zero, zero, zero]
    direction = [zero + 1.0, zero, zero]
    found = [zero, zero, zero]
    norm = g[0, 0]
    for iteration in range(3):
        image = image_of(direction)
        if iteration == 0:
            image = [image[0], image[1], zero, zero]
        elif iteration == 1:
            image = [image[0], image[1], image[2], zero]
        step = norm / form(direction, image)
        found = [f if d is zero else f + step * d for f, d in zip(found, direction)]
        res = [r if m is zero else r - step * m for r, m in zip(res, image)]
        if iteration < 2:
            after = form(res[:3], res[:3])
            ratio = after / norm
            direction = [r if d is zero else r + ratio * d for r, d in zip(res, direction)]
            norm = after

    for c in range(comps):
        def spread(value):
            return jnp.broadcast_to(jnp.sum(jnp.where(at_lane == c, value, 0.0), axis=1, keepdims=True), (Y, Z))

        fx = [spread(f) for f in found]
        fres = [spread(r) for r in res]
        for x in range(X):
            p = [S[c, x, 0:Y, 0:Z] for S in (S0, S1, S2)] + [S3[c, x]]
            x_ref[c, x] = fx[0] * p[0] + fx[1] * p[1] + fx[2] * p[2]
            r_ref[c, x] = fres[0] * p[0] + fres[1] * p[1] + fres[2] * p[2] + fres[3] * p[3]

    for copy, moved in copies:
        pl.when(exists(moved))(copy.wait_send)


def solution(mesh):
    sizes = tuple(mesh.shape[a] for a in AXES)
    groups = groups_of(sizes)

    def body(velocity, diffusion):
        comps, X, Y, Z = velocity.shape
        XR, YR, ZR = X + 2 * MARGIN, Y + 2 * MARGIN, 2 * Z
        f32 = jnp.float32
        whole = pltpu.VMEM((comps, XR, YR, ZR), f32)
        packed = pltpu.VMEM((comps, 8, Z), f32)
        counts = [len(offsets_of(sizes, group)) + 1 for group in groups]
        out = jax.ShapeDtypeStruct(velocity.shape, f32)
        return pl.pallas_call(
            functools.partial(kernel, sizes),
            out_shape=(out, out),
            in_specs=[pl.BlockSpec(memory_space=pltpu.SMEM), pl.BlockSpec(memory_space=pltpu.VMEM)],
            out_specs=(pl.BlockSpec(memory_space=pltpu.VMEM), pl.BlockSpec(memory_space=pltpu.VMEM)),
            scratch_shapes=[
                whole, whole, whole, whole,
                pltpu.VMEM((comps, X, Y, Z), f32),
                pltpu.VMEM((YR, ZR), f32),
                pltpu.VMEM((comps, X, MARGIN, Z), f32),
                pltpu.VMEM((comps, X, MARGIN, Z), f32),
                pltpu.VMEM((comps, XR, MARGIN, Z), f32),
                pltpu.VMEM((comps, XR, MARGIN, Z), f32),
                packed, packed, packed, packed,
                pltpu.VMEM((9, comps, 8, Z), f32),
                pltpu.VMEM((1, Z), f32),
                *[pltpu.VMEM((count, 1, Z), f32) for count in counts],
                pltpu.SemaphoreType.DMA((18,)),
                pltpu.SemaphoreType.DMA((18,)),
                pltpu.SemaphoreType.DMA((len(groups),)),
                pltpu.SemaphoreType.DMA((len(groups),)),
            ],
            compiler_params=pltpu.CompilerParams(collective_id=0, has_side_effects=True),
        )(diffusion, velocity)

    return jax.shard_map(
        body,
        mesh=mesh,
        in_specs=(P(None, "gx", "gy", "gz"), P()),
        out_specs=(P(None, "gx", "gy", "gz"), P(None, "gx", "gy", "gz")),
        check_vma=False,
    )
```

```python
import functools
import itertools

import jax
import jax.numpy as jnp
from jax import lax
from jax.experimental import pallas as pl
from jax.experimental.pallas import tpu as pltpu
from jax.sharding import PartitionSpec as P

AXES = ("gx", "gy", "gz")
MESH_IDS = pl.DeviceIdType.MESH
MARGIN = 4
PAIRS = ((0, 0), (0, 1), (1, 1), (0, 2), (1, 2), (2, 2), (2, 3))
time_step = 0.25
ONE_SHOT = 64
GRANT = 16 * 1024 * 1024


def around(sizes, moved):
    return tuple(lax.rem(lax.axis_index(a) + o, s) for a, o, s in zip(AXES, moved, sizes))


def groups_of(sizes):
    total = sizes[0] * sizes[1] * sizes[2]
    if total <= ONE_SHOT:
        return [(0, 1, 2)]
    return [(0,), (1,), (2,)]


def offsets_of(sizes, group):
    ranges = [range(sizes[k]) if k in group else range(1) for k in range(3)]
    return [o for o in itertools.product(*ranges) if any(o)]


def slot_of(sizes, group):
    slot = 0
    for k in group:
        slot = slot * sizes[k] + lax.axis_index(AXES[k])
    return slot


def kernel(sizes, diff_hbm, v_hbm, x_ref, r_ref, diff_ref, F, S0, S1, S2, S3, mask, SL, SH, RL, RH, pack, zlow, zhigh, Q, QR, row, *rest):
    groups = groups_of(sizes)
    gathered, (fs, fr, gs, gr, ins) = rest[: len(groups)], rest[len(groups):]
    comps, X, Y, Z = v_hbm.shape
    XR, YR, ZR = X + 2 * MARGIN, Y + 2 * MARGIN, 2 * Z
    tiles = Y // 8
    here = [lax.axis_index(a) for a in AXES]

    def exists(moved):
        ok = None
        for k in range(3):
            if moved[k]:
                place = here[k] + moved[k]
                one = (place >= 0) & (place < sizes[k])
                ok = one if ok is None else ok & one
        return ok

    peers = set()
    for group in groups:
        peers.update(offsets_of(sizes, group))
    for dx, dy in itertools.product((-1, 0, 1), (-1, 0, 1)):
        moved = (dx % sizes[0], dy % sizes[1], 0)
        if any(moved):
            peers.add(moved)
    peers = sorted(peers, key=lambda o: -sum(min(m, s - m) for m, s in zip(o, sizes)))
    barrier = pltpu.get_barrier_semaphore()

    for moved in peers:
        pl.semaphore_signal(barrier, inc=1, device_id=around(sizes, moved), device_id_type=MESH_IDS)
    own_cells = pltpu.make_async_copy(v_hbm, F.at[:, 0:X, 0:Y, 0:Z], ins.at[0])
    own_cells.start()
    own_diff = pltpu.make_async_copy(diff_hbm, diff_ref, ins.at[1])
    own_diff.start()

    def missing(moved):
        return pl.when(jnp.logical_not(exists(moved)))

    for c in range(comps):
        F[c, X:XR, :, Z:ZR] = jnp.zeros((XR - X, YR, Z), jnp.float32)

    @missing((1, 0, 0))
    def _():
        for c in range(comps):
            F[c, X : X + MARGIN, 0:Y, 0:Z] = jnp.zeros((MARGIN, Y, Z), jnp.float32)

    @missing((-1, 0, 0))
    def _():
        for c in range(comps):
            F[c, X + MARGIN : XR, 0:Y, 0:Z] = jnp.zeros((MARGIN, Y, Z), jnp.float32)

    D = MARGIN - 1
    for dy, ref in ((-1, RL), (1, RH)):
        for dx, first, count in ((0, 0, X), (1, X, D), (-1, XR - D, D)):
            @missing((dx, dy, 0))
            def _(ref=ref, first=first, count=count):
                for c in range(comps):
                    ref[c, first : first + count] = jnp.zeros((count, MARGIN, Z), jnp.float32)

    for dx, dy in itertools.product((-1, 0, 1), (-1, 0, 1)):
        if dx or dy:
            @missing((dx, dy, 0))
            def _(at=(dx + 1) * 3 + dy + 1):
                QR[at] = jnp.zeros((comps, 8, Z), jnp.float32)

    for dz, ref in ((-1, zlow), (1, zhigh)):
        @missing((0, 0, dz))
        def _(ref=ref):
            ref[...] = jnp.zeros((comps, 8, Z), jnp.float32)

    yy = lax.broadcasted_iota(jnp.int32, (YR, ZR), 0)
    zz = lax.broadcasted_iota(jnp.int32, (YR, ZR), 1)
    yy = jnp.where(yy >= Y + MARGIN, yy - YR, yy) + here[1] * Y
    zz = jnp.where(zz >= Z + Z // 2, zz - ZR, zz) + here[2] * Z
    inside = (yy >= 0) & (yy < Y * sizes[1]) & (zz >= 0) & (zz < Z * sizes[2])
    mask[...] = jnp.where(inside, 1.0, 0.0).astype(jnp.float32)
    own_cells.wait()

    lane = lax.broadcasted_iota(jnp.int32, (8, Z), 1)
    sub = lax.broadcasted_iota(jnp.int32, (8, Z), 0)
    for c in range(comps):
        packed = jnp.zeros((8, Z), jnp.float32)
        for x in range(X):
            for t in range(tiles):
                g = x * tiles + t
                rolled = pltpu.roll(F[c, x, 8 * t : 8 * t + 8, 0:Z], (8 * g + MARGIN) % Z, 1)
                packed = jnp.where(lane // 8 == g, rolled, packed)
        pack[c] = packed
        SL[c] = F[c, 0:X, 0:MARGIN, 0:Z]
        SH[c] = F[c, 0:X, Y - MARGIN : Y, 0:Z]
    pl.semaphore_wait(barrier, len(peers))

    copies = []

    def send(src, dst, moved):
        k = len(copies)
        copy = pltpu.make_async_remote_copy(
            src_ref=src, dst_ref=dst, send_sem=fs.at[k], recv_sem=fr.at[k],
            device_id=tuple(h + m for h, m in zip(here, moved)), device_id_type=MESH_IDS,
        )
        copies.append((copy, moved))
        pl.when(exists(moved))(copy.start)

    def received(which):
        for copy, moved in which:
            pl.when(exists(tuple(-m for m in moved)))(copy.wait_recv)

    send(pack, zhigh, (0, 0, -1))
    send(pack, zlow, (0, 0, 1))
    z_copies = copies[:]
    send(SL, RH.at[:, 0:X], (0, -1, 0))
    send(SH, RL.at[:, 0:X], (0, 1, 0))
    for dx in (-1, 1):
        planes = pl.ds(0, D) if dx < 0 else pl.ds(X - D, D)
        landing = pl.ds(X, D) if dx < 0 else pl.ds(XR - D, D)
        send(SL.at[:, planes], RH.at[:, landing], (dx, -1, 0))
        send(SH.at[:, planes], RL.at[:, landing], (dx, 1, 0))
    send(F.at[:, 0:MARGIN, 0:Y, 0:Z], F.at[:, X : X + MARGIN, 0:Y, 0:Z], (-1, 0, 0))
    send(F.at[:, X - MARGIN : X, 0:Y, 0:Z], F.at[:, X + MARGIN : XR, 0:Y, 0:Z], (1, 0, 0))
    face_copies = copies[len(z_copies):]

    received(z_copies)
    for c in range(comps):
        Q[c] = jnp.where(lane % 8 < MARGIN, zlow[c], zhigh[c])
    steps = [m for m in itertools.product((-1, 0, 1), (-1, 0, 1)) if any(m)]
    for dx, dy in sorted(steps, key=lambda m: -abs(m[1])):
        send(Q, QR.at[(1 - dx) * 3 + (1 - dy)], (dx, dy, 0))
    q_copies = copies[len(z_copies) + len(face_copies):]
    own = 4
    for c in range(comps):
        for x in range(X):
            for t in range(tiles):
                g = x * tiles + t
                F[c, x, 8 * t : 8 * t + 8, Z:ZR] = pltpu.roll(Q[c], (Z - MARGIN - 8 * g) % Z, 1)

    received(face_copies)
    rows_of_y = [x for x in range(XR) if x < X + D or x >= XR - D]
    for c in range(comps):
        for x in rows_of_y:
            F[c, x, Y : Y + MARGIN, 0:Z] = RH[c, x]
            F[c, x, Y + MARGIN : YR, 0:Z] = RL[c, x]
        for x in (X + D, XR - D - 1):
            F[c, x, Y:YR, 0:Z] = jnp.zeros((YR - Y, Z), jnp.float32)
    received(q_copies)

    for c in range(comps):
        for x in rows_of_y:
            dx, at = (0, x) if x < X else ((1, x - X) if x < X + D else (-1, x - MARGIN - MARGIN))
            base = (dx + 1) * 3 + 1
            if dx:
                for t in range(tiles):
                    g = at * tiles + t
                    F[c, x, 8 * t : 8 * t + 8, Z:ZR] = pltpu.roll(QR[base, c], (Z - MARGIN - 8 * g) % Z, 1)
            above = pltpu.roll(QR[base + 1, c], (Z - MARGIN - 8 * (at * tiles)) % Z, 1)
            below = pltpu.roll(QR[base - 1, c], (Z - MARGIN - 8 * (at * tiles + tiles - 1)) % Z, 1)
            F[c, x, Y:YR, Z:ZR] = jnp.where(sub < MARGIN, above, below)

    def ring(i):
        return lax.rem(i, XR)

    def plane_mask(i):
        place = here[0] * X + i
        xin = (place >= XR) & (place < X * sizes[0] + XR)
        return mask[...] * jnp.where(xin, 1.0, 0.0).astype(jnp.float32)

    def section_plane(i, carry):
        at, after, before = ring(i), ring(i + 1), ring(i - 1)
        inner = plane_mask(i)
        v = [F[c, at] for c in range(comps)]
        va = [F[c, after] for c in range(comps)]
        vb = [F[c, before] for c in range(comps)]
        for c in range(comps):
            total = va[0] * va[c] - vb[0] * vb[c]
            fy = v[1] * v[c]
            total = total + (pltpu.roll(fy, YR - 1, 0) - pltpu.roll(fy, 1, 0))
            fz = v[2] * v[c]
            total = total + (pltpu.roll(fz, ZR - 1, 1) - pltpu.roll(fz, 1, 1))
            S0[c, at] = (v[c] - (0.5 * time_step) * total) * inner
        return carry

    lax.fori_loop(XR - D, XR + X + D, section_plane, 0, unroll=True)

    def beside(ref, c, i):
        f = ref[c, ring(i)]
        total = ref[c, ring(i + 1)] + ref[c, ring(i - 1)]
        total = total + (pltpu.roll(f, YR - 1, 0) + pltpu.roll(f, 1, 0))
        return total + (pltpu.roll(f, ZR - 1, 1) + pltpu.roll(f, 1, 1))

    def first_plane(i, carry):
        inner = plane_mask(i)
        for c in range(comps):
            S1[c, ring(i)] = beside(S0, c, i) * inner
        return carry

    lax.fori_loop(XR - 2, XR + X + 2, first_plane, 0, unroll=True)

    def second_plane(i, carry):
        inner = plane_mask(i)
        for c in range(comps):
            S2[c, ring(i)] = beside(S1, c, i) * inner - 6.0 * S0[c, ring(i)]
        return carry

    lax.fori_loop(XR - 1, XR + X + 1, second_plane, 0, unroll=True)

    def third_plane(i, sums):
        sums = list(sums)
        at = i - XR
        for c in range(comps):
            p = [S[c, at, 0:Y, 0:Z] for S in (S0, S1, S2)]
            p.append(beside(S2, c, i)[0:Y, 0:Z] - 9.0 * p[1])
            S3[c, at] = p[3]
            for k, (a, b) in enumerate(PAIRS):
                both = p[a] * p[b]
                part = both[0:8]
                for t in range(1, tiles):
                    part = part + both[8 * t : 8 * t + 8]
                sums[k * comps + c] = sums[k * comps + c] + part
        return tuple(sums)

    sums = lax.fori_loop(XR, XR + X, third_plane, (jnp.zeros((8, Z), jnp.float32),) * (comps * len(PAIRS)), unroll=True)
    line = jnp.zeros((8, Z), jnp.float32)
    for k, part in enumerate(sums):
        line = jnp.where(lane == k, jnp.sum(part, axis=1, keepdims=True), line)
    line = jnp.sum(line, axis=0, keepdims=True)

    order = 0
    for group, landing in zip(groups, gathered):
        mine = slot_of(sizes, group)
        row[...] = line
        landing[mine] = line
        offsets = [o for o in peers if o in offsets_of(sizes, group)]
        for moved in offsets:
            pltpu.make_async_remote_copy(
                src_ref=row, dst_ref=landing.at[mine], send_sem=gs.at[order], recv_sem=gr.at[order],
                device_id=around(sizes, moved), device_id_type=MESH_IDS,
            ).start()
        many = landing.at[pl.ds(0, len(offsets))]
        pltpu.make_async_copy(many, many, gr.at[order]).wait()
        line = landing[0]
        for k in range(1, len(offsets) + 1):
            line = line + landing[k]
        pltpu.make_async_copy(many, many, gs.at[order]).wait()
        order += 1

    g = {}
    for k, (a, b) in enumerate(PAIRS):
        value = line if k == 0 else pltpu.roll(line, Z - k * comps, 1)
        g[a, b] = g[b, a] = value
    g[0, 3] = g[1, 2] - 9.0 * g[0, 1]
    g[1, 3] = g[2, 2] + 6.0 * g[0, 2] - 9.0 * g[1, 1]
    at_lane = lax.broadcasted_iota(jnp.int32, (1, Z), 1)
    own_diff.wait()
    coef = jnp.full((1, Z), 1.0, jnp.float32)
    for c in range(comps):
        coef = jnp.where(at_lane == c, diff_ref[c], coef)
    diagonal = 1.0 + 6.0 * coef
    zero = jnp.zeros((1, Z), jnp.float32)

    def image_of(d):
        return [
            diagonal * d[0] - 6.0 * coef * d[1],
            diagonal * d[1] - coef * (d[0] + 9.0 * d[2]),
            diagonal * d[2] - coef * d[1],
            -coef * d[2],
        ]

    def form(a, b):
        total = None
        for i, left in enumerate(a):
            for j, right in enumerate(b):
                if left is zero or right is zero:
                    continue
                term = left * right * g[i, j]
                total = term if total is None else total + term
        return total

    res = [zero + 1.0, zero, zero, zero]
    direction = [zero + 1.0, zero, zero]
    found = [zero, zero, zero]
    norm = g[0, 0]
    for iteration in range(3):
        image = image_of(direction)
        if iteration == 0:
            image = [image[0], image[1], zero, zero]
        elif iteration == 1:
            image = [image[0], image[1], image[2], zero]
        step = norm / form(direction, image)
        found = [f if d is zero else f + step * d for f, d in zip(found, direction)]
        res = [r if m is zero else r - step * m for r, m in zip(res, image)]
        if iteration < 2:
            after = form(res[:3], res[:3])
            ratio = after / norm
            direction = [r if d is zero else r + ratio * d for r, d in zip(res, direction)]
            norm = after

    for c in range(comps):
        def spread(value):
            return jnp.broadcast_to(jnp.sum(jnp.where(at_lane == c, value, 0.0), axis=1, keepdims=True), (Y, Z))

        fx = [spread(f) for f in found]
        fres = [spread(r) for r in res]
        for x in range(X):
            p = [S[c, x, 0:Y, 0:Z] for S in (S0, S1, S2)] + [S3[c, x]]
            x_ref[c, x] = fx[0] * p[0] + fx[1] * p[1] + fx[2] * p[2]
            r_ref[c, x] = fres[0] * p[0] + fres[1] * p[1] + fres[2] * p[2] + fres[3] * p[3]

    for copy, moved in copies:
        pl.when(exists(moved))(copy.wait_send)


def solution(mesh):
    sizes = tuple(mesh.shape[a] for a in AXES)
    groups = groups_of(sizes)

    def body(velocity, diffusion):
        comps, X, Y, Z = velocity.shape
        XR, YR, ZR = X + 2 * MARGIN, Y + 2 * MARGIN, 2 * Z
        f32 = jnp.float32
        whole = pltpu.VMEM((comps, XR, YR, ZR), f32)
        packed = pltpu.VMEM((comps, 8, Z), f32)
        counts = [len(offsets_of(sizes, group)) + 1 for group in groups]
        out = jax.ShapeDtypeStruct(velocity.shape, f32)
        return pl.pallas_call(
            functools.partial(kernel, sizes),
            out_shape=(out, out),
            in_specs=[pl.BlockSpec(memory_space=pltpu.HBM)] * 2,
            out_specs=(pl.BlockSpec(memory_space=pltpu.VMEM), pl.BlockSpec(memory_space=pltpu.VMEM)),
            scratch_shapes=[
                pltpu.SMEM((comps,), f32),
                whole, whole, whole, whole,
                pltpu.VMEM((comps, X, Y, Z), f32),
                pltpu.VMEM((YR, ZR), f32),
                pltpu.VMEM((comps, X, MARGIN, Z), f32),
                pltpu.VMEM((comps, X, MARGIN, Z), f32),
                pltpu.VMEM((comps, XR, MARGIN, Z), f32),
                pltpu.VMEM((comps, XR, MARGIN, Z), f32),
                packed, packed, packed, packed,
                pltpu.VMEM((9, comps, 8, Z), f32),
                pltpu.VMEM((1, Z), f32),
                *[pltpu.VMEM((count, 1, Z), f32) for count in counts],
                pltpu.SemaphoreType.DMA((18,)),
                pltpu.SemaphoreType.DMA((18,)),
                pltpu.SemaphoreType.DMA((len(groups),)),
                pltpu.SemaphoreType.DMA((len(groups),)),
                pltpu.SemaphoreType.DMA((2,)),
            ],
            compiler_params=pltpu.CompilerParams(collective_id=0, has_side_effects=True, vmem_limit_bytes=GRANT),
        )(diffusion, velocity)

    return jax.shard_map(
        body,
        mesh=mesh,
        in_specs=(P(None, "gx", "gy", "gz"), P()),
        out_specs=(P(None, "gx", "gy", "gz"), P(None, "gx", "gy", "gz")),
        check_vma=False,
    )
```

```python
import functools
import itertools

import jax
import jax.numpy as jnp
from jax import lax
from jax.experimental import pallas as pl
from jax.experimental.pallas import tpu as pltpu
from jax.sharding import PartitionSpec as P

AXES = ("gx", "gy", "gz")
MESH_IDS = pl.DeviceIdType.MESH
MARGIN = 4
PAIRS = ((0, 0), (0, 1), (1, 1), (0, 2), (1, 2), (2, 2), (2, 3))
time_step = 0.25
ONE_SHOT = 64
GRANT = 66000000


def around(sizes, moved):
    return tuple(lax.rem(lax.axis_index(a) + o, s) for a, o, s in zip(AXES, moved, sizes))


def groups_of(sizes):
    total = sizes[0] * sizes[1] * sizes[2]
    if total <= ONE_SHOT:
        return [(0, 1, 2)]
    return [(0,), (1,), (2,)]


def offsets_of(sizes, group):
    ranges = [range(sizes[k]) if k in group else range(1) for k in range(3)]
    return [o for o in itertools.product(*ranges) if any(o)]


def slot_of(sizes, group):
    slot = 0
    for k in group:
        slot = slot * sizes[k] + lax.axis_index(AXES[k])
    return slot


def kernel(sizes, diff_hbm, v_hbm, x_ref, r_ref, diff_ref, F, S0, S1, S2, S3, mask, SL, SH, RL, RH, pack, zlow, zhigh, Q, QR, row, *rest):
    groups = groups_of(sizes)
    gathered, (fs, fr, gs, gr, ins, waves) = rest[: len(groups)], rest[len(groups):]
    comps, X, Y, Z = v_hbm.shape
    XR, YR, ZR = X + 2 * MARGIN, Y + 2 * MARGIN, 2 * Z
    tiles = Y // 8
    here = [lax.axis_index(a) for a in AXES]

    def exists(moved):
        ok = None
        for k in range(3):
            if moved[k]:
                place = here[k] + moved[k]
                one = (place >= 0) & (place < sizes[k])
                ok = one if ok is None else ok & one
        return ok

    peers = set()
    for group in groups:
        peers.update(offsets_of(sizes, group))
    for dx, dy in itertools.product((-1, 0, 1), (-1, 0, 1)):
        moved = (dx % sizes[0], dy % sizes[1], 0)
        if any(moved):
            peers.add(moved)
    peers = sorted(peers, key=lambda o: -sum(min(m, s - m) for m, s in zip(o, sizes)))
    barrier = pltpu.get_barrier_semaphore()
    relayed = len(groups) == 1
    greeted = [o for o in peers if not (relayed and o[2])]
    beyond = ((0, 0, -1), (0, 0, 1)) if relayed else ()

    def shifted(moved):
        return tuple(h + m for h, m in zip(here, moved))

    own_cells = pltpu.make_async_copy(v_hbm, F.at[:, 0:X, 0:Y, 0:Z], ins.at[0])
    own_cells.start()
    own_diff = pltpu.make_async_copy(diff_hbm, diff_ref, ins.at[1])
    own_diff.start()

    expected = len(greeted)
    for moved in greeted:
        pl.semaphore_signal(barrier, inc=1, device_id=around(sizes, moved), device_id_type=MESH_IDS)
    for moved in beyond:
        @pl.when(exists(moved))
        def _(moved=moved):
            pl.semaphore_signal(barrier, inc=1, device_id=shifted(moved), device_id_type=MESH_IDS)

        expected = expected + exists(moved).astype(jnp.int32)

    def announce(wave):
        for k, moved in enumerate(beyond):
            @pl.when(exists(moved))
            def _(k=k, moved=moved):
                pl.semaphore_signal(waves.at[wave, k], inc=1, device_id=shifted(moved), device_id_type=MESH_IDS)

    def heard(wave):
        for k, moved in enumerate(beyond):
            @pl.when(exists(tuple(-m for m in moved)))
            def _(k=k):
                pl.semaphore_wait(waves.at[wave, k], 1)

    last_wave = sizes[2] - 1
    def missing(moved):
        return pl.when(jnp.logical_not(exists(moved)))

    for c in range(comps):
        F[c, X:XR, :, Z:ZR] = jnp.zeros((XR - X, YR, Z), jnp.float32)

    @missing((1, 0, 0))
    def _():
        for c in range(comps):
            F[c, X : X + MARGIN, 0:Y, 0:Z] = jnp.zeros((MARGIN, Y, Z), jnp.float32)

    @missing((-1, 0, 0))
    def _():
        for c in range(comps):
            F[c, X + MARGIN : XR, 0:Y, 0:Z] = jnp.zeros((MARGIN, Y, Z), jnp.float32)

    D = MARGIN - 1
    for dy, ref in ((-1, RL), (1, RH)):
        for dx, first, count in ((0, 0, X), (1, X, D), (-1, XR - D, D)):
            @missing((dx, dy, 0))
            def _(ref=ref, first=first, count=count):
                for c in range(comps):
                    ref[c, first : first + count] = jnp.zeros((count, MARGIN, Z), jnp.float32)

    for dx, dy in itertools.product((-1, 0, 1), (-1, 0, 1)):
        if dx or dy:
            @missing((dx, dy, 0))
            def _(at=(dx + 1) * 3 + dy + 1):
                QR[at] = jnp.zeros((comps, 8, Z), jnp.float32)

    for dz, ref in ((-1, zlow), (1, zhigh)):
        @missing((0, 0, dz))
        def _(ref=ref):
            ref[...] = jnp.zeros((comps, 8, Z), jnp.float32)

    yy = lax.broadcasted_iota(jnp.int32, (YR, ZR), 0)
    zz = lax.broadcasted_iota(jnp.int32, (YR, ZR), 1)
    yy = jnp.where(yy >= Y + MARGIN, yy - YR, yy) + here[1] * Y
    zz = jnp.where(zz >= Z + Z // 2, zz - ZR, zz) + here[2] * Z
    inside = (yy >= 0) & (yy < Y * sizes[1]) & (zz >= 0) & (zz < Z * sizes[2])
    mask[...] = jnp.where(inside, 1.0, 0.0).astype(jnp.float32)
    own_cells.wait()

    lane = lax.broadcasted_iota(jnp.int32, (8, Z), 1)
    sub = lax.broadcasted_iota(jnp.int32, (8, Z), 0)
    for c in range(comps):
        packed = jnp.zeros((8, Z), jnp.float32)
        for x in range(X):
            for t in range(tiles):
                g = x * tiles + t
                rolled = pltpu.roll(F[c, x, 8 * t : 8 * t + 8, 0:Z], (8 * g + MARGIN) % Z, 1)
                packed = jnp.where(lane // 8 == g, rolled, packed)
        pack[c] = packed
        SL[c] = F[c, 0:X, 0:MARGIN, 0:Z]
        SH[c] = F[c, 0:X, Y - MARGIN : Y, 0:Z]
    pl.semaphore_wait(barrier, expected)

    copies = []

    def send(src, dst, moved):
        k = len(copies)
        copy = pltpu.make_async_remote_copy(
            src_ref=src, dst_ref=dst, send_sem=fs.at[k], recv_sem=fr.at[k],
            device_id=tuple(h + m for h, m in zip(here, moved)), device_id_type=MESH_IDS,
        )
        copies.append((copy, moved))
        pl.when(exists(moved))(copy.start)

    def received(which):
        for copy, moved in which:
            pl.when(exists(tuple(-m for m in moved)))(copy.wait_recv)

    send(pack, zhigh, (0, 0, -1))
    send(pack, zlow, (0, 0, 1))
    z_copies = copies[:]
    send(SL, RH.at[:, 0:X], (0, -1, 0))
    send(SH, RL.at[:, 0:X], (0, 1, 0))
    for dx in (-1, 1):
        planes = pl.ds(0, D) if dx < 0 else pl.ds(X - D, D)
        landing = pl.ds(X, D) if dx < 0 else pl.ds(XR - D, D)
        send(SL.at[:, planes], RH.at[:, landing], (dx, -1, 0))
        send(SH.at[:, planes], RL.at[:, landing], (dx, 1, 0))
    send(F.at[:, 0:MARGIN, 0:Y, 0:Z], F.at[:, X : X + MARGIN, 0:Y, 0:Z], (-1, 0, 0))
    send(F.at[:, X - MARGIN : X, 0:Y, 0:Z], F.at[:, X + MARGIN : XR, 0:Y, 0:Z], (1, 0, 0))
    face_copies = copies[len(z_copies):]

    received(z_copies)
    if last_wave >= 2:
        announce(2)
    for c in range(comps):
        Q[c] = jnp.where(lane % 8 < MARGIN, zlow[c], zhigh[c])
    steps = [m for m in itertools.product((-1, 0, 1), (-1, 0, 1)) if any(m)]
    for dx, dy in sorted(steps, key=lambda m: -abs(m[1])):
        send(Q, QR.at[(1 - dx) * 3 + (1 - dy)], (dx, dy, 0))
    q_copies = copies[len(z_copies) + len(face_copies):]
    own = 4
    for c in range(comps):
        for x in range(X):
            for t in range(tiles):
                g = x * tiles + t
                F[c, x, 8 * t : 8 * t + 8, Z:ZR] = pltpu.roll(Q[c], (Z - MARGIN - 8 * g) % Z, 1)

    received(face_copies)
    if last_wave >= 2:
        heard(2)
    if last_wave >= 3:
        announce(3)
    rows_of_y = [x for x in range(XR) if x < X + D or x >= XR - D]
    for c in range(comps):
        for x in rows_of_y:
            F[c, x, Y : Y + MARGIN, 0:Z] = RH[c, x]
            F[c, x, Y + MARGIN : YR, 0:Z] = RL[c, x]
        for x in (X + D, XR - D - 1):
            F[c, x, Y:YR, 0:Z] = jnp.zeros((YR - Y, Z), jnp.float32)
    received(q_copies)

    for c in range(comps):
        for x in rows_of_y:
            dx, at = (0, x) if x < X else ((1, x - X) if x < X + D else (-1, x - MARGIN - MARGIN))
            base = (dx + 1) * 3 + 1
            if dx:
                for t in range(tiles):
                    g = at * tiles + t
                    F[c, x, 8 * t : 8 * t + 8, Z:ZR] = pltpu.roll(QR[base, c], (Z - MARGIN - 8 * g) % Z, 1)
            above = pltpu.roll(QR[base + 1, c], (Z - MARGIN - 8 * (at * tiles)) % Z, 1)
            below = pltpu.roll(QR[base - 1, c], (Z - MARGIN - 8 * (at * tiles + tiles - 1)) % Z, 1)
            F[c, x, Y:YR, Z:ZR] = jnp.where(sub < MARGIN, above, below)

    def ring(i):
        return lax.rem(i, XR)

    def plane_mask(i):
        place = here[0] * X + i
        xin = (place >= XR) & (place < X * sizes[0] + XR)
        return mask[...] * jnp.where(xin, 1.0, 0.0).astype(jnp.float32)

    def section_plane(i, carry):
        at, after, before = ring(i), ring(i + 1), ring(i - 1)
        inner = plane_mask(i)
        v = [F[c, at] for c in range(comps)]
        va = [F[c, after] for c in range(comps)]
        vb = [F[c, before] for c in range(comps)]
        for c in range(comps):
            total = va[0] * va[c] - vb[0] * vb[c]
            fy = v[1] * v[c]
            total = total + (pltpu.roll(fy, YR - 1, 0) - pltpu.roll(fy, 1, 0))
            fz = v[2] * v[c]
            total = total + (pltpu.roll(fz, ZR - 1, 1) - pltpu.roll(fz, 1, 1))
            S0[c, at] = (v[c] - (0.5 * time_step) * total) * inner
        return carry

    lax.fori_loop(XR - D, XR + X + D, section_plane, 0, unroll=True)

    def beside(ref, c, i):
        f = ref[c, ring(i)]
        total = ref[c, ring(i + 1)] + ref[c, ring(i - 1)]
        total = total + (pltpu.roll(f, YR - 1, 0) + pltpu.roll(f, 1, 0))
        return total + (pltpu.roll(f, ZR - 1, 1) + pltpu.roll(f, 1, 1))

    def first_plane(i, carry):
        inner = plane_mask(i)
        for c in range(comps):
            S1[c, ring(i)] = beside(S0, c, i) * inner
        return carry

    lax.fori_loop(XR - 2, XR + X + 2, first_plane, 0, unroll=True)

    def second_plane(i, carry):
        inner = plane_mask(i)
        for c in range(comps):
            S2[c, ring(i)] = beside(S1, c, i) * inner - 6.0 * S0[c, ring(i)]
        return carry

    lax.fori_loop(XR - 1, XR + X + 1, second_plane, 0, unroll=True)

    def third_plane(i, sums):
        sums = list(sums)
        at = i - XR
        for c in range(comps):
            p = [S[c, at, 0:Y, 0:Z] for S in (S0, S1, S2)]
            p.append(beside(S2, c, i)[0:Y, 0:Z] - 9.0 * p[1])
            S3[c, at] = p[3]
            for k, (a, b) in enumerate(PAIRS):
                both = p[a] * p[b]
                part = both[0:8]
                for t in range(1, tiles):
                    part = part + both[8 * t : 8 * t + 8]
                sums[k * comps + c] = sums[k * comps + c] + part
        return tuple(sums)

    sums = lax.fori_loop(XR, XR + X, third_plane, (jnp.zeros((8, Z), jnp.float32),) * (comps * len(PAIRS)), unroll=True)
    line = jnp.zeros((8, Z), jnp.float32)
    for k, part in enumerate(sums):
        line = jnp.where(lane == k, jnp.sum(part, axis=1, keepdims=True), line)
    line = jnp.sum(line, axis=0, keepdims=True)

    for wave in range(3, last_wave + 1):
        heard(wave)
        if wave < last_wave:
            announce(wave + 1)
    order = 0
    for group, landing in zip(groups, gathered):
        mine = slot_of(sizes, group)
        row[...] = line
        landing[mine] = line
        offsets = [o for o in peers if o in offsets_of(sizes, group)]
        for moved in offsets:
            pltpu.make_async_remote_copy(
                src_ref=row, dst_ref=landing.at[mine], send_sem=gs.at[order], recv_sem=gr.at[order],
                device_id=around(sizes, moved), device_id_type=MESH_IDS,
            ).start()
        many = landing.at[pl.ds(0, len(offsets))]
        pltpu.make_async_copy(many, many, gr.at[order]).wait()
        line = landing[0]
        for k in range(1, len(offsets) + 1):
            line = line + landing[k]
        pltpu.make_async_copy(many, many, gs.at[order]).wait()
        order += 1

    g = {}
    for k, (a, b) in enumerate(PAIRS):
        value = line if k == 0 else pltpu.roll(line, Z - k * comps, 1)
        g[a, b] = g[b, a] = value
    g[0, 3] = g[1, 2] - 9.0 * g[0, 1]
    g[1, 3] = g[2, 2] + 6.0 * g[0, 2] - 9.0 * g[1, 1]
    at_lane = lax.broadcasted_iota(jnp.int32, (1, Z), 1)
    own_diff.wait()
    coef = jnp.full((1, Z), 1.0, jnp.float32)
    for c in range(comps):
        coef = jnp.where(at_lane == c, diff_ref[c], coef)
    diagonal = 1.0 + 6.0 * coef
    zero = jnp.zeros((1, Z), jnp.float32)

    def image_of(d):
        return [
            diagonal * d[0] - 6.0 * coef * d[1],
            diagonal * d[1] - coef * (d[0] + 9.0 * d[2]),
            diagonal * d[2] - coef * d[1],
            -coef * d[2],
        ]

    def form(a, b):
        total = None
        for i, left in enumerate(a):
            for j, right in enumerate(b):
                if left is zero or right is zero:
                    continue
                term = left * right * g[i, j]
                total = term if total is None else total + term
        return total

    res = [zero + 1.0, zero, zero, zero]
    direction = [zero + 1.0, zero, zero]
    found = [zero, zero, zero]
    norm = g[0, 0]
    for iteration in range(3):
        image = image_of(direction)
        if iteration == 0:
            image = [image[0], image[1], zero, zero]
        elif iteration == 1:
            image = [image[0], image[1], image[2], zero]
        step = norm / form(direction, image)
        found = [f if d is zero else f + step * d for f, d in zip(found, direction)]
        res = [r if m is zero else r - step * m for r, m in zip(res, image)]
        if iteration < 2:
            after = form(res[:3], res[:3])
            ratio = after / norm
            direction = [r if d is zero else r + ratio * d for r, d in zip(res, direction)]
            norm = after

    for c in range(comps):
        def spread(value):
            return jnp.broadcast_to(jnp.sum(jnp.where(at_lane == c, value, 0.0), axis=1, keepdims=True), (Y, Z))

        fx = [spread(f) for f in found]
        fres = [spread(r) for r in res]
        for x in range(X):
            p = [S[c, x, 0:Y, 0:Z] for S in (S0, S1, S2)] + [S3[c, x]]
            x_ref[c, x] = fx[0] * p[0] + fx[1] * p[1] + fx[2] * p[2]
            r_ref[c, x] = fres[0] * p[0] + fres[1] * p[1] + fres[2] * p[2] + fres[3] * p[3]

    for copy, moved in copies:
        pl.when(exists(moved))(copy.wait_send)


def solution(mesh):
    sizes = tuple(mesh.shape[a] for a in AXES)
    groups = groups_of(sizes)

    def body(velocity, diffusion):
        comps, X, Y, Z = velocity.shape
        XR, YR, ZR = X + 2 * MARGIN, Y + 2 * MARGIN, 2 * Z
        f32 = jnp.float32
        whole = pltpu.VMEM((comps, XR, YR, ZR), f32)
        packed = pltpu.VMEM((comps, 8, Z), f32)
        counts = [len(offsets_of(sizes, group)) + 1 for group in groups]
        out = pltpu.VMEM(velocity.shape, f32)
        return pl.pallas_call(
            functools.partial(kernel, sizes),
            out_shape=(out, out),
            in_specs=[pl.BlockSpec(memory_space=pltpu.HBM)] * 2,
            out_specs=(pl.BlockSpec(memory_space=pltpu.VMEM), pl.BlockSpec(memory_space=pltpu.VMEM)),
            scratch_shapes=[
                pltpu.SMEM((comps,), f32),
                whole, whole, whole, whole,
                pltpu.VMEM((comps, X, Y, Z), f32),
                pltpu.VMEM((YR, ZR), f32),
                pltpu.VMEM((comps, X, MARGIN, Z), f32),
                pltpu.VMEM((comps, X, MARGIN, Z), f32),
                pltpu.VMEM((comps, XR, MARGIN, Z), f32),
                pltpu.VMEM((comps, XR, MARGIN, Z), f32),
                packed, packed, packed, packed,
                pltpu.VMEM((9, comps, 8, Z), f32),
                pltpu.VMEM((1, Z), f32),
                *[pltpu.VMEM((count, 1, Z), f32) for count in counts],
                pltpu.SemaphoreType.DMA((18,)),
                pltpu.SemaphoreType.DMA((18,)),
                pltpu.SemaphoreType.DMA((len(groups),)),
                pltpu.SemaphoreType.DMA((len(groups),)),
                pltpu.SemaphoreType.DMA((2,)),
                pltpu.SemaphoreType.REGULAR((sizes[2], 2)),
            ],
            compiler_params=pltpu.CompilerParams(collective_id=0, has_side_effects=True, vmem_limit_bytes=GRANT),
        )(diffusion, velocity)

    return jax.shard_map(
        body,
        mesh=mesh,
        in_specs=(P(None, "gx", "gy", "gz"), P()),
        out_specs=(P(None, "gx", "gy", "gz"), P(None, "gx", "gy", "gz")),
        check_vma=False,
    )
```

```python
import functools
import itertools

import jax
import jax.numpy as jnp
from jax import lax
from jax.experimental import pallas as pl
from jax.experimental.pallas import tpu as pltpu
from jax.sharding import PartitionSpec as P

AXES = ("gx", "gy", "gz")
MESH_IDS = pl.DeviceIdType.MESH
MARGIN = 4
PAIRS = ((0, 0), (0, 1), (1, 1), (0, 2), (1, 2), (2, 2), (2, 3))
time_step = 0.25
ONE_SHOT = 64
GRANT = 66000000


def around(sizes, moved):
    return tuple(lax.rem(lax.axis_index(a) + o, s) for a, o, s in zip(AXES, moved, sizes))


def groups_of(sizes):
    total = sizes[0] * sizes[1] * sizes[2]
    if total <= ONE_SHOT:
        return [(0, 1, 2)]
    return [(0,), (1,), (2,)]


def offsets_of(sizes, group):
    ranges = [range(sizes[k]) if k in group else range(1) for k in range(3)]
    return [o for o in itertools.product(*ranges) if any(o)]


def slot_of(sizes, group):
    slot = 0
    for k in group:
        slot = slot * sizes[k] + lax.axis_index(AXES[k])
    return slot


def kernel(sizes, diff_hbm, v_hbm, x_ref, r_ref, diff_ref, F, S0, S1, S2, S3, mask, SL, SH, RL, RH, pack, zlow, zhigh, Q, QR, row, *rest):
    groups = groups_of(sizes)
    gathered, (fs, fr, gs, gr, ins, waves) = rest[: len(groups)], rest[len(groups):]
    comps, X, Y, Z = v_hbm.shape
    XR, YR, ZR = X + 2 * MARGIN, Y + 2 * MARGIN, 2 * Z
    tiles = Y // 8
    here = [lax.axis_index(a) for a in AXES]

    def exists(moved):
        ok = None
        for k in range(3):
            if moved[k]:
                place = here[k] + moved[k]
                one = (place >= 0) & (place < sizes[k])
                ok = one if ok is None else ok & one
        return ok

    peers = set()
    for group in groups:
        peers.update(offsets_of(sizes, group))
    for dx, dy in itertools.product((-1, 0, 1), (-1, 0, 1)):
        moved = (dx % sizes[0], dy % sizes[1], 0)
        if any(moved):
            peers.add(moved)
    peers = sorted(peers, key=lambda o: -sum(min(m, s - m) for m, s in zip(o, sizes)))
    barrier = pltpu.get_barrier_semaphore()
    relayed = len(groups) == 1
    greeted = [o for o in peers if not (relayed and o[2])]
    beyond = ((0, 0, -1), (0, 0, 1)) if relayed else ()

    def shifted(moved):
        return tuple(h + m for h, m in zip(here, moved))

    own_cells = pltpu.make_async_copy(v_hbm, F.at[:, 0:X, 0:Y, 0:Z], ins.at[0])
    own_cells.start()
    own_diff = pltpu.make_async_copy(diff_hbm, diff_ref, ins.at[1])
    own_diff.start()

    expected = len(greeted)
    for moved in greeted:
        pl.semaphore_signal(barrier, inc=1, device_id=around(sizes, moved), device_id_type=MESH_IDS)
    for moved in beyond:
        @pl.when(exists(moved))
        def _(moved=moved):
            pl.semaphore_signal(barrier, inc=1, device_id=shifted(moved), device_id_type=MESH_IDS)

        expected = expected + exists(moved).astype(jnp.int32)

    def announce(wave):
        for k, moved in enumerate(beyond):
            @pl.when(exists(moved))
            def _(k=k, moved=moved):
                pl.semaphore_signal(waves.at[wave, k], inc=1, device_id=shifted(moved), device_id_type=MESH_IDS)

    def heard(wave):
        for k, moved in enumerate(beyond):
            @pl.when(exists(tuple(-m for m in moved)))
            def _(k=k):
                pl.semaphore_wait(waves.at[wave, k], 1)

    last_wave = sizes[2] - 1
    def missing(moved):
        return pl.when(jnp.logical_not(exists(moved)))

    for c in range(comps):
        F[c, X:XR, :, Z:ZR] = jnp.zeros((XR - X, YR, Z), jnp.float32)

    @missing((1, 0, 0))
    def _():
        for c in range(comps):
            F[c, X : X + MARGIN, 0:Y, 0:Z] = jnp.zeros((MARGIN, Y, Z), jnp.float32)

    @missing((-1, 0, 0))
    def _():
        for c in range(comps):
            F[c, X + MARGIN : XR, 0:Y, 0:Z] = jnp.zeros((MARGIN, Y, Z), jnp.float32)

    D = MARGIN - 1
    for dy, ref in ((-1, RL), (1, RH)):
        for dx, first, count in ((0, 0, X), (1, X, D), (-1, XR - D, D)):
            @missing((dx, dy, 0))
            def _(ref=ref, first=first, count=count):
                for c in range(comps):
                    ref[c, first : first + count] = jnp.zeros((count, MARGIN, Z), jnp.float32)

    for dx, dy in itertools.product((-1, 0, 1), (-1, 0, 1)):
        if dx or dy:
            @missing((dx, dy, 0))
            def _(at=(dx + 1) * 3 + dy + 1):
                QR[at] = jnp.zeros((comps, 8, Z), jnp.float32)

    for dz, ref in ((-1, zlow), (1, zhigh)):
        @missing((0, 0, dz))
        def _(ref=ref):
            ref[...] = jnp.zeros((comps, 8, Z), jnp.float32)

    yy = lax.broadcasted_iota(jnp.int32, (YR, ZR), 0)
    zz = lax.broadcasted_iota(jnp.int32, (YR, ZR), 1)
    yy = jnp.where(yy >= Y + MARGIN, yy - YR, yy) + here[1] * Y
    zz = jnp.where(zz >= Z + Z // 2, zz - ZR, zz) + here[2] * Z
    inside = (yy >= 0) & (yy < Y * sizes[1]) & (zz >= 0) & (zz < Z * sizes[2])
    mask[...] = jnp.where(inside, 1.0, 0.0).astype(jnp.float32)
    own_cells.wait()

    lane = lax.broadcasted_iota(jnp.int32, (8, Z), 1)
    sub = lax.broadcasted_iota(jnp.int32, (8, Z), 0)
    for c in range(comps):
        packed = jnp.zeros((8, Z), jnp.float32)
        for x in range(X):
            for t in range(tiles):
                g = x * tiles + t
                rolled = pltpu.roll(F[c, x, 8 * t : 8 * t + 8, 0:Z], (8 * g + MARGIN) % Z, 1)
                packed = jnp.where(lane // 8 == g, rolled, packed)
        pack[c] = packed
    pl.semaphore_wait(barrier, expected)

    copies = []

    def send(src, dst, moved):
        k = len(copies)
        copy = pltpu.make_async_remote_copy(
            src_ref=src, dst_ref=dst, send_sem=fs.at[k], recv_sem=fr.at[k],
            device_id=tuple(h + m for h, m in zip(here, moved)), device_id_type=MESH_IDS,
        )
        copies.append((copy, moved))
        pl.when(exists(moved))(copy.start)

    def received(which):
        for copy, moved in which:
            pl.when(exists(tuple(-m for m in moved)))(copy.wait_recv)

    send(pack, zhigh, (0, 0, -1))
    send(pack, zlow, (0, 0, 1))
    z_copies = copies[:]
    for c in range(comps):
        SL[c] = F[c, 0:X, 0:MARGIN, 0:Z]
        SH[c] = F[c, 0:X, Y - MARGIN : Y, 0:Z]
    send(SL, RH.at[:, 0:X], (0, -1, 0))
    send(SH, RL.at[:, 0:X], (0, 1, 0))
    send(F.at[:, 0:MARGIN, 0:Y, 0:Z], F.at[:, X : X + MARGIN, 0:Y, 0:Z], (-1, 0, 0))
    send(F.at[:, X - MARGIN : X, 0:Y, 0:Z], F.at[:, X + MARGIN : XR, 0:Y, 0:Z], (1, 0, 0))
    face_copies = copies[len(z_copies):]

    received(z_copies)
    if last_wave >= 2:
        announce(2)
    for c in range(comps):
        Q[c] = jnp.where(lane % 8 < MARGIN, zlow[c], zhigh[c])
    steps = [m for m in itertools.product((-1, 0, 1), (-1, 0, 1)) if any(m)]
    for dx, dy in sorted(steps, key=lambda m: -abs(m[1])):
        send(Q, QR.at[(1 - dx) * 3 + (1 - dy)], (dx, dy, 0))
    q_copies = copies[len(z_copies) + len(face_copies):]
    for dx in (-1, 1):
        planes = pl.ds(0, D) if dx < 0 else pl.ds(X - D, D)
        landing = pl.ds(X, D) if dx < 0 else pl.ds(XR - D, D)
        send(SL.at[:, planes], RH.at[:, landing], (dx, -1, 0))
        send(SH.at[:, planes], RL.at[:, landing], (dx, 1, 0))
    late_copies = copies[len(z_copies) + len(face_copies) + len(q_copies) :]
    for c in range(comps):
        for x in range(X):
            for t in range(tiles):
                g = x * tiles + t
                F[c, x, 8 * t : 8 * t + 8, Z:ZR] = pltpu.roll(Q[c], (Z - MARGIN - 8 * g) % Z, 1)

    received(face_copies)
    received(late_copies)
    if last_wave >= 2:
        heard(2)
    if last_wave >= 3:
        announce(3)
    rows_of_y = [x for x in range(XR) if x < X + D or x >= XR - D]
    for c in range(comps):
        for x in rows_of_y:
            F[c, x, Y : Y + MARGIN, 0:Z] = RH[c, x]
            F[c, x, Y + MARGIN : YR, 0:Z] = RL[c, x]
        for x in (X + D, XR - D - 1):
            F[c, x, Y:YR, 0:Z] = jnp.zeros((YR - Y, Z), jnp.float32)
    received(q_copies)

    for c in range(comps):
        for x in rows_of_y:
            dx, at = (0, x) if x < X else ((1, x - X) if x < X + D else (-1, x - MARGIN - MARGIN))
            base = (dx + 1) * 3 + 1
            if dx:
                for t in range(tiles):
                    g = at * tiles + t
                    F[c, x, 8 * t : 8 * t + 8, Z:ZR] = pltpu.roll(QR[base, c], (Z - MARGIN - 8 * g) % Z, 1)
            above = pltpu.roll(QR[base + 1, c], (Z - MARGIN - 8 * (at * tiles)) % Z, 1)
            below = pltpu.roll(QR[base - 1, c], (Z - MARGIN - 8 * (at * tiles + tiles - 1)) % Z, 1)
            F[c, x, Y:YR, Z:ZR] = jnp.where(sub < MARGIN, above, below)

    def ring(i):
        return lax.rem(i, XR)

    def plane_mask(i):
        place = here[0] * X + i
        xin = (place >= XR) & (place < X * sizes[0] + XR)
        return mask[...] * jnp.where(xin, 1.0, 0.0).astype(jnp.float32)

    def section_plane(i, carry):
        at, after, before = ring(i), ring(i + 1), ring(i - 1)
        inner = plane_mask(i)
        v = [F[c, at] for c in range(comps)]
        va = [F[c, after] for c in range(comps)]
        vb = [F[c, before] for c in range(comps)]
        for c in range(comps):
            total = va[0] * va[c] - vb[0] * vb[c]
            fy = v[1] * v[c]
            total = total + (pltpu.roll(fy, YR - 1, 0) - pltpu.roll(fy, 1, 0))
            fz = v[2] * v[c]
            total = total + (pltpu.roll(fz, ZR - 1, 1) - pltpu.roll(fz, 1, 1))
            S0[c, at] = (v[c] - (0.5 * time_step) * total) * inner
        return carry

    lax.fori_loop(XR - D, XR + X + D, section_plane, 0, unroll=True)

    def beside(ref, c, i):
        f = ref[c, ring(i)]
        total = ref[c, ring(i + 1)] + ref[c, ring(i - 1)]
        total = total + (pltpu.roll(f, YR - 1, 0) + pltpu.roll(f, 1, 0))
        return total + (pltpu.roll(f, ZR - 1, 1) + pltpu.roll(f, 1, 1))

    def first_plane(i, carry):
        inner = plane_mask(i)
        for c in range(comps):
            S1[c, ring(i)] = beside(S0, c, i) * inner
        return carry

    lax.fori_loop(XR - 2, XR + X + 2, first_plane, 0, unroll=True)

    def second_plane(i, carry):
        inner = plane_mask(i)
        for c in range(comps):
            S2[c, ring(i)] = beside(S1, c, i) * inner - 6.0 * S0[c, ring(i)]
        return carry

    lax.fori_loop(XR - 1, XR + X + 1, second_plane, 0, unroll=True)

    def third_plane(i, sums):
        sums = list(sums)
        at = i - XR
        for c in range(comps):
            p = [S[c, at, 0:Y, 0:Z] for S in (S0, S1, S2)]
            p.append(beside(S2, c, i)[0:Y, 0:Z] - 9.0 * p[1])
            S3[c, at] = p[3]
            for k, (a, b) in enumerate(PAIRS):
                both = p[a] * p[b]
                part = both[0:8]
                for t in range(1, tiles):
                    part = part + both[8 * t : 8 * t + 8]
                sums[k * comps + c] = sums[k * comps + c] + part
        return tuple(sums)

    sums = lax.fori_loop(XR, XR + X, third_plane, (jnp.zeros((8, Z), jnp.float32),) * (comps * len(PAIRS)), unroll=True)
    line = jnp.zeros((8, Z), jnp.float32)
    for k, part in enumerate(sums):
        line = jnp.where(lane == k, jnp.sum(part, axis=1, keepdims=True), line)
    line = jnp.sum(line, axis=0, keepdims=True)

    for wave in range(3, last_wave + 1):
        heard(wave)
        if wave < last_wave:
            announce(wave + 1)
    order = 0
    for group, landing in zip(groups, gathered):
        mine = slot_of(sizes, group)
        row[...] = line
        landing[mine] = line
        offsets = [o for o in peers if o in offsets_of(sizes, group)]
        for moved in offsets:
            pltpu.make_async_remote_copy(
                src_ref=row, dst_ref=landing.at[mine], send_sem=gs.at[order], recv_sem=gr.at[order],
                device_id=around(sizes, moved), device_id_type=MESH_IDS,
            ).start()
        many = landing.at[pl.ds(0, len(offsets))]
        pltpu.make_async_copy(many, many, gr.at[order]).wait()
        line = landing[0]
        for k in range(1, len(offsets) + 1):
            line = line + landing[k]
        pltpu.make_async_copy(many, many, gs.at[order]).wait()
        order += 1

    g = {}
    for k, (a, b) in enumerate(PAIRS):
        value = line if k == 0 else pltpu.roll(line, Z - k * comps, 1)
        g[a, b] = g[b, a] = value
    g[0, 3] = g[1, 2] - 9.0 * g[0, 1]
    g[1, 3] = g[2, 2] + 6.0 * g[0, 2] - 9.0 * g[1, 1]
    at_lane = lax.broadcasted_iota(jnp.int32, (1, Z), 1)
    own_diff.wait()
    coef = jnp.full((1, Z), 1.0, jnp.float32)
    for c in range(comps):
        coef = jnp.where(at_lane == c, diff_ref[c], coef)
    diagonal = 1.0 + 6.0 * coef
    zero = jnp.zeros((1, Z), jnp.float32)

    def image_of(d):
        return [
            diagonal * d[0] - 6.0 * coef * d[1],
            diagonal * d[1] - coef * (d[0] + 9.0 * d[2]),
            diagonal * d[2] - coef * d[1],
            -coef * d[2],
        ]

    def form(a, b):
        total = None
        for i, left in enumerate(a):
            for j, right in enumerate(b):
                if left is zero or right is zero:
                    continue
                term = left * right * g[i, j]
                total = term if total is None else total + term
        return total

    res = [zero + 1.0, zero, zero, zero]
    direction = [zero + 1.0, zero, zero]
    found = [zero, zero, zero]
    norm = g[0, 0]
    for iteration in range(3):
        image = image_of(direction)
        if iteration == 0:
            image = [image[0], image[1], zero, zero]
        elif iteration == 1:
            image = [image[0], image[1], image[2], zero]
        step = norm / form(direction, image)
        found = [f if d is zero else f + step * d for f, d in zip(found, direction)]
        res = [r if m is zero else r - step * m for r, m in zip(res, image)]
        if iteration < 2:
            after = form(res[:3], res[:3])
            ratio = after / norm
            direction = [r if d is zero else r + ratio * d for r, d in zip(res, direction)]
            norm = after

    for c in range(comps):
        def spread(value):
            return jnp.broadcast_to(jnp.sum(jnp.where(at_lane == c, value, 0.0), axis=1, keepdims=True), (Y, Z))

        fx = [spread(f) for f in found]
        fres = [spread(r) for r in res]
        for x in range(X):
            p = [S[c, x, 0:Y, 0:Z] for S in (S0, S1, S2)] + [S3[c, x]]
            x_ref[c, x] = fx[0] * p[0] + fx[1] * p[1] + fx[2] * p[2]
            r_ref[c, x] = fres[0] * p[0] + fres[1] * p[1] + fres[2] * p[2] + fres[3] * p[3]

    for copy, moved in copies:
        pl.when(exists(moved))(copy.wait_send)


def solution(mesh):
    sizes = tuple(mesh.shape[a] for a in AXES)
    groups = groups_of(sizes)

    def body(velocity, diffusion):
        comps, X, Y, Z = velocity.shape
        XR, YR, ZR = X + 2 * MARGIN, Y + 2 * MARGIN, 2 * Z
        f32 = jnp.float32
        whole = pltpu.VMEM((comps, XR, YR, ZR), f32)
        packed = pltpu.VMEM((comps, 8, Z), f32)
        counts = [len(offsets_of(sizes, group)) + 1 for group in groups]
        out = pltpu.VMEM(velocity.shape, f32)
        return pl.pallas_call(
            functools.partial(kernel, sizes),
            out_shape=(out, out),
            in_specs=[pl.BlockSpec(memory_space=pltpu.HBM)] * 2,
            out_specs=(pl.BlockSpec(memory_space=pltpu.VMEM), pl.BlockSpec(memory_space=pltpu.VMEM)),
            scratch_shapes=[
                pltpu.SMEM((comps,), f32),
                whole, whole, whole, whole,
                pltpu.VMEM((comps, X, Y, Z), f32),
                pltpu.VMEM((YR, ZR), f32),
                pltpu.VMEM((comps, X, MARGIN, Z), f32),
                pltpu.VMEM((comps, X, MARGIN, Z), f32),
                pltpu.VMEM((comps, XR, MARGIN, Z), f32),
                pltpu.VMEM((comps, XR, MARGIN, Z), f32),
                packed, packed, packed, packed,
                pltpu.VMEM((9, comps, 8, Z), f32),
                pltpu.VMEM((1, Z), f32),
                *[pltpu.VMEM((count, 1, Z), f32) for count in counts],
                pltpu.SemaphoreType.DMA((18,)),
                pltpu.SemaphoreType.DMA((18,)),
                pltpu.SemaphoreType.DMA((len(groups),)),
                pltpu.SemaphoreType.DMA((len(groups),)),
                pltpu.SemaphoreType.DMA((2,)),
                pltpu.SemaphoreType.REGULAR((sizes[2], 2)),
            ],
            compiler_params=pltpu.CompilerParams(collective_id=0, has_side_effects=True, vmem_limit_bytes=GRANT),
        )(diffusion, velocity)

    return jax.shard_map(
        body,
        mesh=mesh,
        in_specs=(P(None, "gx", "gy", "gz"), P()),
        out_specs=(P(None, "gx", "gy", "gz"), P(None, "gx", "gy", "gz")),
        check_vma=False,
    )
```
